8 devices in a mesh: model: 2 (over z, y), data: 4 (over x, core).
Axes of the slice: x: 2, y: 2, z: 1, core: 2. Of those that a mesh axis runs over, the one named last changes fastest.
Arguments:
- x_tokens: bfloat16 [16384, 2048], P('data')
- dy_tokens: bfloat16 [16384, 2048], P('data')
- w_col: bfloat16 [2, 2048, 2048], P(None, None, 'model')
- w_row: bfloat16 [2, 2048, 2048], P(None, 'model')
- a_old_col: float32 [2, 2048, 2048], replicated
- s_old_col: float32 [2, 2048, 1024], P(None, 'model')
- a_old_row: float32 [2, 2048, 1024], P(None, 'model')
- s_old_row: float32 [2, 2048, 2048], replicated
- a_inv_col: float32 [2, 2048, 2048], replicated
- s_inv_col: float32 [2, 2048, 1024], P(None, 'model')
- a_inv_row: float32 [2, 2048, 1024], P(None, 'model')
- s_inv_row: float32 [2, 2048, 2048], replicated
Outputs:
- output 1: float32 [2, 2048, 2048], P(None, None, 'model')
- output 2: float32 [2, 2048, 2048], P(None, 'model')
- output 3: float32 [2, 2048, 2048], replicated
- output 4: float32 [2, 2048, 1024], P(None, 'model')
- output 5: float32 [2, 2048, 1024], P(None, 'model')
- output 6: float32 [2, 2048, 2048], replicated
All inputs are finite; a program needn't handle non-finite values.
Results may differ from the reference program's by a relative error of at most 0.00457.
Values are sent between devices in bfloat16 or wider.
A program may use at most 1.25 GiB of HBM per device.

```python
import math
import jax
import jax.numpy as jnp
from jax import lax

HIDDEN = 2048
TOKENS_DEV = 4096
DATA_WAYS = 4
MODEL_WAYS = 2
BATCH_ROWS = TOKENS_DEV * DATA_WAYS
BLOCK_DIM = HIDDEN // MODEL_WAYS
FACTOR_DECAY = 0.8
GELU_SCALE = math.sqrt(2.0 / math.pi)
GELU_CUBIC = 0.044715
EXACT = lax.Precision.HIGHEST


def gelu_value(pre_act):
    tanh_arg = GELU_SCALE * (pre_act + GELU_CUBIC * pre_act * pre_act * pre_act)
    return 0.5 * pre_act * (1.0 + jnp.tanh(tanh_arg))


def gelu_slope(pre_act):
    tanh_arg = GELU_SCALE * (pre_act + GELU_CUBIC * pre_act * pre_act * pre_act)
    tanh_val = jnp.tanh(tanh_arg)
    return 0.5 * (1.0 + tanh_val) + 0.5 * pre_act * (1.0 - tanh_val * tanh_val) * GELU_SCALE * (1.0 + 3.0 * GELU_CUBIC * pre_act * pre_act)


def activate(pre_act):
    return gelu_value(pre_act.astype(jnp.float32)).astype(jnp.bfloat16)


def back_gate(grad_act, pre_act):
    return (grad_act.astype(jnp.float32) * gelu_slope(pre_act.astype(jnp.float32))).astype(jnp.bfloat16)


def sym_draw(rand_key, lead_count, mat_dim, spread):
    diag_key, noise_key = jax.random.split(rand_key)
    diag_vals = jax.random.uniform(diag_key, (lead_count, mat_dim), jnp.float32, 0.5, 1.5)
    sym_noise = jax.random.normal(noise_key, (lead_count, mat_dim, mat_dim), jnp.float32)
    sym_noise = (sym_noise + jnp.swapaxes(sym_noise, 1, 2)) * (spread / math.sqrt(2.0 * mat_dim))
    return sym_noise + diag_vals[:, :, None] * jnp.eye(mat_dim, dtype=jnp.float32)


def block_draw(rand_key, spread):
    return sym_draw(rand_key, 2 * MODEL_WAYS, BLOCK_DIM, spread).reshape(2, HIDDEN, BLOCK_DIM)


def token_draw(rand_key):
    mean_key, scale_key, base_key = jax.random.split(rand_key, 3)
    shard_mean = jax.random.normal(mean_key, (DATA_WAYS, 1, HIDDEN), jnp.float32) * (0.5 * HIDDEN ** -0.25)
    shard_scale = jnp.exp2(jax.random.uniform(scale_key, (DATA_WAYS, 1, 1), jnp.float32, -1.0, 1.0))
    base_vals = jax.random.normal(base_key, (DATA_WAYS, TOKENS_DEV, HIDDEN), jnp.float32)
    return (base_vals * shard_scale + shard_mean).reshape(BATCH_ROWS, HIDDEN).astype(jnp.bfloat16)


def setup_inputs(seed: int = 0) -> dict:
    key_list = jax.random.split(jax.random.key(seed), 12)
    weight_scale = HIDDEN ** -0.5
    return {
        'x_tokens': token_draw(key_list[0]),
        'dy_tokens': token_draw(key_list[1]),
        'w_col': (jax.random.normal(key_list[2], (2, HIDDEN, HIDDEN), jnp.float32) * weight_scale).astype(jnp.bfloat16),
        'w_row': (jax.random.normal(key_list[3], (2, HIDDEN, HIDDEN), jnp.float32) * weight_scale).astype(jnp.bfloat16),
        'a_old_col': sym_draw(key_list[4], 2, HIDDEN, 0.3),
        's_old_col': block_draw(key_list[5], 0.3),
        'a_old_row': block_draw(key_list[6], 0.3),
        's_old_row': sym_draw(key_list[7], 2, HIDDEN, 0.3),
        'a_inv_col': sym_draw(key_list[8], 2, HIDDEN, 0.2),
        's_inv_col': block_draw(key_list[9], 0.2),
        'a_inv_row': block_draw(key_list[10], 0.2),
        's_inv_row': sym_draw(key_list[11], 2, HIDDEN, 0.2),
    }


def gram_mat(left_mat, right_mat):
    return jnp.dot(left_mat.T, right_mat, preferred_element_type=jnp.float32) / BATCH_ROWS


def block_gram(left_mat, right_mat):
    left_blocks = jnp.swapaxes(left_mat.reshape(BATCH_ROWS, MODEL_WAYS, BLOCK_DIM), 0, 1)
    right_blocks = jnp.swapaxes(right_mat.reshape(BATCH_ROWS, MODEL_WAYS, BLOCK_DIM), 0, 1)
    blocks = lax.map(lambda block_pair: jnp.dot(block_pair[0].T, block_pair[1], preferred_element_type=jnp.float32), (left_blocks, right_blocks))
    return blocks.reshape(HIDDEN, BLOCK_DIM) / BATCH_ROWS


def precondition_col(a_inv, grad_mat, s_inv_blocks):
    left_done = jnp.dot(a_inv, grad_mat, precision=EXACT).reshape(HIDDEN, MODEL_WAYS, BLOCK_DIM)
    right_blocks = s_inv_blocks.reshape(MODEL_WAYS, BLOCK_DIM, BLOCK_DIM)
    return jnp.einsum('dmi,mij->dmj', left_done, right_blocks, precision=EXACT).reshape(HIDDEN, HIDDEN)


def precondition_row(a_inv_blocks, grad_mat, s_inv):
    left_blocks = a_inv_blocks.reshape(MODEL_WAYS, BLOCK_DIM, BLOCK_DIM)
    left_done = jnp.einsum('mij,mjk->mik', left_blocks, grad_mat.reshape(MODEL_WAYS, BLOCK_DIM, HIDDEN), precision=EXACT).reshape(HIDDEN, HIDDEN)
    return jnp.dot(left_done, s_inv, precision=EXACT)


def blend_factor(old_mats, first_new, second_new):
    return FACTOR_DECAY * old_mats + (1.0 - FACTOR_DECAY) * jnp.stack([first_new, second_new])


def reference(x_tokens, dy_tokens, w_col, w_row, a_old_col, s_old_col, a_old_row, s_old_row, a_inv_col, s_inv_col, a_inv_row, s_inv_row):
    z_one = jnp.dot(x_tokens, w_col[0], preferred_element_type=jnp.float32).astype(jnp.bfloat16)
    h_one = activate(z_one)
    z_two = jnp.dot(h_one, w_row[0], preferred_element_type=jnp.float32).astype(jnp.bfloat16)
    h_two = activate(z_two)
    z_three = jnp.dot(h_two, w_col[1], preferred_element_type=jnp.float32).astype(jnp.bfloat16)
    h_three = activate(z_three)
    g_three = back_gate(jnp.dot(dy_tokens, w_row[1].T, preferred_element_type=jnp.float32).astype(jnp.bfloat16), z_three)
    g_two = back_gate(jnp.dot(g_three, w_col[1].T, preferred_element_type=jnp.float32).astype(jnp.bfloat16), z_two)
    g_one = back_gate(jnp.dot(g_two, w_row[0].T, preferred_element_type=jnp.float32).astype(jnp.bfloat16), z_one)
    u_col = jnp.stack([
        precondition_col(a_inv_col[0], gram_mat(x_tokens, g_one), s_inv_col[0]),
        precondition_col(a_inv_col[1], gram_mat(h_two, g_three), s_inv_col[1]),
    ])
    u_row = jnp.stack([
        precondition_row(a_inv_row[0], gram_mat(h_one, g_two), s_inv_row[0]),
        precondition_row(a_inv_row[1], gram_mat(h_three, dy_tokens), s_inv_row[1]),
    ])
    a_new_col = blend_factor(a_old_col, gram_mat(x_tokens, x_tokens), gram_mat(h_two, h_two))
    s_new_col = blend_factor(s_old_col, block_gram(g_one, g_one), block_gram(g_three, g_three))
    a_new_row = blend_factor(a_old_row, block_gram(h_one, h_one), block_gram(h_three, h_three))
    s_new_row = blend_factor(s_old_row, gram_mat(g_two, g_two), gram_mat(dy_tokens, dy_tokens))
    return (u_col, u_row, a_new_col, s_new_col, a_new_row, s_new_row)
```

```python
import math
import jax
import jax.numpy as jnp
from jax import lax
from jax.sharding import PartitionSpec as P

FACTOR_DECAY = 0.8
GELU_SCALE = math.sqrt(2.0 / math.pi)
GELU_CUBIC = 0.044715
EXACT = lax.Precision.HIGHEST
TN_DIMS = (((0,), (0,)), ((), ()))
NT_DIMS = (((1,), (1,)), ((), ()))
ALL_AXES = ('model', 'data')
SUB = 512
LOCAL_ORDER = ((2, 0, 1, 3), (1, 2, 3, 0))
GLOBAL_ORDER = ((1, 2, 0, 3), (3, 0, 1, 2))


def gelu_value(pre_act):
    tanh_arg = GELU_SCALE * (pre_act + GELU_CUBIC * pre_act * pre_act * pre_act)
    return 0.5 * pre_act * (1.0 + jnp.tanh(tanh_arg))


def gelu_slope(pre_act):
    tanh_arg = GELU_SCALE * (pre_act + GELU_CUBIC * pre_act * pre_act * pre_act)
    tanh_val = jnp.tanh(tanh_arg)
    return 0.5 * (1.0 + tanh_val) + 0.5 * pre_act * (1.0 - tanh_val * tanh_val) * GELU_SCALE * (1.0 + 3.0 * GELU_CUBIC * pre_act * pre_act)


def activate(pre_act):
    return gelu_value(pre_act.astype(jnp.float32)).astype(jnp.bfloat16)


def back_gate(grad_act, pre_act):
    return (grad_act.astype(jnp.float32) * gelu_slope(pre_act.astype(jnp.float32))).astype(jnp.bfloat16)


def matmul(left_mat, right_mat):
    return jnp.dot(left_mat, right_mat, preferred_element_type=jnp.float32)


def matmul_tn(left_mat, right_mat):
    return lax.dot_general(left_mat, right_mat, TN_DIMS, preferred_element_type=jnp.float32)


def matmul_nt(left_mat, right_mat):
    return lax.dot_general(left_mat, right_mat, NT_DIMS, preferred_element_type=jnp.float32)


def exact_dot(left_mat, right_mat):
    return jnp.dot(left_mat, right_mat, precision=EXACT, preferred_element_type=jnp.float32)


def exact_tn(left_mat, right_mat):
    return lax.dot_general(left_mat, right_mat, TN_DIMS, precision=EXACT, preferred_element_type=jnp.float32)


def reorder(mat, axis, order, half):
    picks = [jnp.where(half == 0, zero, one) * SUB for zero, one in zip(*order)]
    return jnp.concatenate([lax.dynamic_slice_in_dim(mat, pick, SUB, axis) for pick in picks], axis)


def full_gram_part(local_mat):
    own_a = local_mat[:, SUB:2 * SUB]
    own_b = local_mat[:, 2 * SUB:3 * SUB]
    return [matmul_tn(own_a, local_mat[:, :3 * SUB]), matmul_tn(own_b, local_mat[:, 2 * SUB:])]


def block_gram_part(own_mat):
    return [matmul_tn(own_mat[:, :SUB], own_mat), matmul_tn(own_mat[:, SUB:], own_mat[:, SUB:])]


def sum_scatter(parts):
    joined = parts[0] if len(parts) == 1 else jnp.concatenate(parts, 1)
    return lax.psum_scatter(joined, 'data', scatter_dimension=0, tiled=True)


def full_symmetric(gathered):
    def piece(half, index):
        return gathered[half * SUB:(half + 1) * SUB, index * SUB:(index + 1) * SUB]
    p02, p00, p01, p11, p13 = [piece(0, index) for index in range(5)]
    p21, p22, p23, p33, p30 = [piece(1, index) for index in range(5)]
    return jnp.concatenate([
        jnp.concatenate([p00, p01, p02, p30.T], 1),
        jnp.concatenate([p01.T, p11, p21.T, p13], 1),
        jnp.concatenate([p02.T, p21, p22, p23], 1),
        jnp.concatenate([p30, p13.T, p23.T, p33], 1),
    ], 0)


def block_symmetric(gathered):
    paa, pab, pbb = [gathered[:, index * SUB:(index + 1) * SUB] for index in range(3)]
    return jnp.concatenate([jnp.concatenate([paa, pab], 1), jnp.concatenate([pab.T, pbb], 1)], 0)


def blend_factor(old_mats, first_new, second_new, inv_rows):
    return FACTOR_DECAY * old_mats + (1.0 - FACTOR_DECAY) * inv_rows * jnp.stack([first_new, second_new])


def solution(mesh):
    data_ways = mesh.shape['data']

    def shard_body(x_tokens, dy_tokens, w_col, w_row, a_old_col, s_old_col, a_old_row, s_old_row, a_inv_col, s_inv_col, a_inv_row, s_inv_row):
        half = lax.axis_index('model')
        quarter = lax.axis_index('data')
        inv_rows = 1.0 / (x_tokens.shape[0] * data_ways)
        hidden = x_tokens.shape[1]
        own_cols = w_col.shape[2]
        piece = own_cols // data_ways

        def col_weight(layer):
            mine = lax.dynamic_slice_in_dim(w_col[layer], quarter * piece, piece, 1)
            every = lax.all_gather(mine, ALL_AXES, axis=0)
            wide = jnp.concatenate([every[index] for index in range(every.shape[0])], 1)
            return reorder(wide, 1, LOCAL_ORDER, half)

        def row_weight(layer):
            mine = lax.dynamic_slice_in_dim(w_row[layer], quarter * piece, piece, 0)
            every = lax.all_gather(mine, ALL_AXES, axis=0, tiled=True)
            return reorder(every, 0, LOCAL_ORDER, half)

        weight_one = col_weight(0)
        weight_two = reorder(row_weight(0), 1, LOCAL_ORDER, half)
        weight_three = reorder(col_weight(1), 0, LOCAL_ORDER, half)
        weight_four = row_weight(1)
        own = slice(SUB, 3 * SUB)

        x_local = reorder(x_tokens, 1, LOCAL_ORDER, half)
        dy_local = reorder(dy_tokens, 1, LOCAL_ORDER, half)
        edge_sum = sum_scatter(full_gram_part(x_local) + full_gram_part(dy_local))

        z_one = matmul(x_tokens, weight_one).astype(jnp.bfloat16)
        h_one = activate(z_one)
        h_one_own = h_one[:, own]
        z_two = matmul(h_one, weight_two).astype(jnp.bfloat16)
        h_two = activate(z_two)
        early_sum = sum_scatter(block_gram_part(h_one_own) + full_gram_part(h_two))
        z_three = matmul(h_two, weight_three).astype(jnp.bfloat16)
        h_three_own = activate(z_three[:, own])
        dw_four = sum_scatter([matmul_tn(h_three_own, dy_tokens)])
        g_three = back_gate(matmul_nt(dy_tokens, weight_four).astype(jnp.bfloat16), z_three)
        g_three_own = g_three[:, own]
        middle_sum = sum_scatter(block_gram_part(h_three_own) + block_gram_part(g_three_own))
        dw_three = sum_scatter([matmul_tn(g_three_own, h_two)])
        g_two = back_gate(matmul_nt(g_three, weight_three).astype(jnp.bfloat16), z_two)
        dw_two = sum_scatter([matmul_tn(h_one_own, g_two)])
        g_one_own = back_gate(matmul_nt(g_two, weight_two[own]).astype(jnp.bfloat16), z_one[:, own])
        dw_one = sum_scatter([matmul_tn(g_one_own, x_tokens)])
        late_sum = sum_scatter(full_gram_part(g_two) + block_gram_part(g_one_own))

        def half_done(grad_piece, inverse, is_local):
            if is_local:
                grad_piece = reorder(grad_piece, 1, GLOBAL_ORDER, half)
            done = exact_dot(grad_piece * inv_rows, inverse)
            return lax.all_gather(done, 'data', axis=0, tiled=True)

        u_row_four = exact_dot(a_inv_row[1], half_done(dw_four, s_inv_row[1], False))
        u_col_three = exact_tn(half_done(dw_three, a_inv_col[1], True), s_inv_col[1])
        u_row_two = exact_dot(a_inv_row[0], half_done(dw_two, s_inv_row[0], True))
        u_col_one = exact_tn(half_done(dw_one, a_inv_col[0], False), s_inv_col[0])
        u_col = jnp.stack([u_col_one, u_col_three])
        u_row = jnp.stack([u_row_two, u_row_four])

        full_cols = 5 * SUB
        block_cols = 3 * SUB
        edge_all = lax.all_gather(edge_sum, ALL_AXES, axis=0, tiled=True)
        h_two_all = lax.all_gather(early_sum[:, block_cols:], ALL_AXES, axis=0, tiled=True)
        g_two_all = lax.all_gather(late_sum[:, :full_cols], ALL_AXES, axis=0, tiled=True)
        middle_all = lax.all_gather(middle_sum, 'data', axis=0, tiled=True)
        outer_all = lax.all_gather(jnp.concatenate([early_sum[:, :block_cols], late_sum[:, full_cols:]], 1), 'data', axis=0, tiled=True)

        a_new_col = blend_factor(a_old_col, full_symmetric(edge_all[:, :full_cols]), full_symmetric(h_two_all), inv_rows)
        s_new_row = blend_factor(s_old_row, full_symmetric(g_two_all), full_symmetric(edge_all[:, full_cols:]), inv_rows)
        a_new_row = blend_factor(a_old_row, block_symmetric(outer_all[:, :block_cols]), block_symmetric(middle_all[:, :block_cols]), inv_rows)
        s_new_col = blend_factor(s_old_col, block_symmetric(outer_all[:, block_cols:]), block_symmetric(middle_all[:, block_cols:]), inv_rows)
        return (u_col, u_row, a_new_col, s_new_col, a_new_row, s_new_row)

    batch_split = P('data', None)
    col_split = P(None, None, 'model')
    row_split = P(None, 'model', None)
    replicated = P()
    return jax.shard_map(
        shard_body,
        mesh=mesh,
        in_specs=(batch_split, batch_split, col_split, row_split, replicated, row_split, row_split, replicated, replicated, row_split, row_split, replicated),
        out_specs=(col_split, row_split, replicated, row_split, row_split, replicated),
        check_vma=False,
    )
```

```python
import functools
import math
import jax
import jax.numpy as jnp
from jax import lax
from jax.experimental import pallas as pl
from jax.experimental.pallas import tpu as pltpu
from jax.sharding import PartitionSpec as P

FACTOR_DECAY = 0.8
GELU_SCALE = math.sqrt(2.0 / math.pi)
GELU_CUBIC = 0.044715
EXACT = lax.Precision.HIGHEST
TN_DIMS = (((0,), (0,)), ((), ()))
NT_DIMS = (((1,), (1,)), ((), ()))
SUB = 512
OWN = slice(SUB, 3 * SUB)
LOCAL_ORDER = ((2, 0, 1, 3), (1, 2, 3, 0))
MODEL_SWAP = ((0, 1), (1, 0))
CHIP_SWAP = ((0, 2), (2, 0), (1, 3), (3, 1))
CORE_SWAP = ((0, 1), (1, 0), (2, 3), (3, 2))
FULL_TABLE = ((0, 1, 0), (0, 2, 0), (0, 0, 0), (1, 4, 1),
              (0, 2, 1), (0, 3, 0), (1, 0, 1), (0, 4, 0),
              (0, 0, 1), (1, 0, 0), (1, 1, 0), (1, 2, 0),
              (1, 4, 0), (0, 4, 1), (1, 2, 1), (1, 3, 0))
BLOCK_TABLE = ((0, 0, 0), (0, 1, 0), (0, 1, 1), (0, 2, 0))


def gelu_value(pre_act):
    tanh_val = jnp.tanh(pre_act * (GELU_SCALE + (GELU_SCALE * GELU_CUBIC * pre_act) * pre_act))
    return 0.5 * pre_act * (1.0 + tanh_val)


def gelu_slope(pre_act):
    square = (3.0 * GELU_CUBIC * pre_act) * pre_act
    tanh_val = jnp.tanh(pre_act * (GELU_SCALE + (GELU_SCALE / 3.0) * square))
    upper = 0.5 + 0.5 * tanh_val
    return upper + ((upper * (1.0 - upper)) * (2.0 * GELU_SCALE * pre_act)) * (1.0 + square)


def activate(pre_act):
    return gelu_value(pre_act.astype(jnp.float32)).astype(jnp.bfloat16)


def back_gate(grad_act, pre_act):
    return (grad_act.astype(jnp.float32) * gelu_slope(pre_act.astype(jnp.float32))).astype(jnp.bfloat16)


def matmul(left_mat, right_mat):
    return jnp.dot(left_mat, right_mat, preferred_element_type=jnp.float32)


def matmul_tn(left_mat, right_mat):
    return lax.dot_general(left_mat, right_mat, TN_DIMS, preferred_element_type=jnp.float32)


def matmul_nt(left_mat, right_mat):
    return lax.dot_general(left_mat, right_mat, NT_DIMS, preferred_element_type=jnp.float32)


def exact_dot(left_mat, right_mat):
    return jnp.dot(left_mat, right_mat, precision=EXACT, preferred_element_type=jnp.float32)


def exact_tn(left_mat, right_mat):
    return lax.dot_general(left_mat, right_mat, TN_DIMS, precision=EXACT, preferred_element_type=jnp.float32)


def reorder(mat, half):
    picks = [jnp.where(half == 0, zero, one) * SUB for zero, one in zip(*LOCAL_ORDER)]
    return jnp.concatenate([lax.dynamic_slice_in_dim(mat, pick, SUB, 1) for pick in picks], 1)


def after(value, *earlier):
    return lax.optimization_barrier((value, *earlier))[0]


def full_gram_part(local_mat):
    own_a = local_mat[:, SUB:2 * SUB]
    own_b = local_mat[:, 2 * SUB:3 * SUB]
    return [matmul_tn(own_a, local_mat[:, :3 * SUB]), matmul_tn(own_b, local_mat[:, 2 * SUB:])]


def block_gram_part(own_mat):
    return [matmul_tn(own_mat[:, :SUB], own_mat), matmul_tn(own_mat[:, SUB:], own_mat[:, SUB:])]


def sum_scatter(part):
    return lax.psum_scatter(part, 'data', scatter_dimension=0, tiled=True)


def spread(piece, over_model):
    found = [piece, lax.ppermute(piece, 'data', CHIP_SWAP)]
    if over_model:
        found += [lax.ppermute(mat, 'model', MODEL_SWAP) for mat in found]
    relayed = [lax.ppermute(mat, 'data', CORE_SWAP) for mat in found]
    return [mat for pair in zip(found, relayed) for mat in pair]


def blend_body(new_scale, blocks, groups, half_tab, piece_tab, flip_tab, place, old_ref, *rest):
    piece_refs, out_ref = rest[:4 * groups], rest[-1]
    entry = pl.program_id(0) * blocks + pl.program_id(1)
    flip = flip_tab[entry]
    distance = lax.bitwise_xor(half_tab[entry], place[0]) if groups == 2 else 0
    part = SUB // 4

    def write(refs, flipped):
        for index, ref in enumerate(refs):
            spot = pl.ds(pl.multiple_of(lax.bitwise_xor(place[1], index) * part, part), part)
            if flipped:
                out_ref[0, :, spot] = FACTOR_DECAY * old_ref[0, :, spot] + new_scale * ref[...].T
            else:
                out_ref[0, spot, :] = FACTOR_DECAY * old_ref[0, spot, :] + new_scale * ref[...]

    for group in range(groups):
        for flipped in (0, 1):
            @pl.when(jnp.logical_and(flip == flipped, distance == group))
            def _():
                write(piece_refs[4 * group:4 * group + 4], flipped)


def blend_layer(old_mats, pieces, first_piece, layer, new_scale, place, partial_out):
    size = old_mats.shape[1]
    blocks = size // SUB
    groups = len(pieces) // 4
    table = FULL_TABLE if blocks == 4 else BLOCK_TABLE
    tables = [jnp.array(column, jnp.int32) for column in zip(*table)] + [place]
    spot = pl.BlockSpec((1, SUB, SUB), lambda row, col, *tabs: (layer, row, col))

    def picked(group):
        def index_map(row, col, halves, names, flips, where):
            entry = row * blocks + col
            needed = lax.bitwise_xor(halves[entry], where[0]) == group if groups == 2 else True
            return 0, first_piece + jnp.where(needed, names[entry], 0)

        return pl.BlockSpec((SUB // 4, SUB), index_map)

    in_specs = [spot] + [picked(index // 4) for index in range(len(pieces))]
    args = [old_mats, *pieces]
    aliases = {}
    if partial_out is not None:
        in_specs.append(pl.BlockSpec(memory_space=pl.ANY))
        args.append(partial_out)
        aliases = {len(tables) + len(args) - 1: 0}
    return pl.pallas_call(
        functools.partial(blend_body, new_scale, blocks, groups),
        grid_spec=pltpu.PrefetchScalarGridSpec(num_scalar_prefetch=len(tables), grid=(blocks, blocks), in_specs=in_specs, out_specs=spot),
        out_shape=jax.ShapeDtypeStruct(old_mats.shape, jnp.float32),
        input_output_aliases=aliases,
        cost_estimate=pl.CostEstimate(flops=3 * size * size, bytes_accessed=12 * size * size, transcendentals=0),
        name='blend_layer',
    )(*tables, *args)


def join_body(place, share_ref, other_ref, *rest):
    out_ref = rest[-1]
    from_share = lax.rem(place[1], 2) == pl.program_id(1)

    @pl.when(from_share)
    def _():
        out_ref[0] = share_ref[...]

    @pl.when(jnp.logical_not(from_share))
    def _():
        out_ref[0] = other_ref[...]


def join_layer(share, other, layer, is_col, place, partial_out):
    rows, cols = share.shape
    step = rows // 4
    shape = (2, 2 * rows, cols) if is_col else (2, rows, 2 * cols)
    taken = pl.BlockSpec((step, cols), lambda row, side, place: (row, 0))
    put = pl.BlockSpec((1, step, cols), lambda row, side, place: (layer, row + 4 * side, 0) if is_col else (layer, row, side))
    in_specs = [taken, taken]
    args = [share, other]
    aliases = {}
    if partial_out is not None:
        in_specs.append(pl.BlockSpec(memory_space=pl.ANY))
        args.append(partial_out)
        aliases = {3: 0}
    return pl.pallas_call(
        join_body,
        grid_spec=pltpu.PrefetchScalarGridSpec(num_scalar_prefetch=1, grid=(4, 2), in_specs=in_specs, out_specs=put),
        out_shape=jax.ShapeDtypeStruct(shape, jnp.float32),
        input_output_aliases=aliases,
        cost_estimate=pl.CostEstimate(flops=2 * rows * cols, bytes_accessed=16 * rows * cols, transcendentals=0),
        name='join_layer',
    )(place, *args)


def solution(mesh):
    data_ways = mesh.shape['data']

    def shard_body(x_tokens, dy_tokens, w_col, w_row, a_old_col, s_old_col, a_old_row, s_old_row, a_inv_col, s_inv_col, a_inv_row, s_inv_row):
        half = lax.axis_index('model')
        quarter = lax.axis_index('data')
        core = lax.rem(quarter, 2)
        inv_rows = 1.0 / (x_tokens.shape[0] * data_ways)
        sent_piece = jnp.where(core == 0, 1 - half, half) * SUB

        place = jnp.stack([half, quarter]).astype(jnp.int32)

        def weight_piece(stack, layer, axis):
            sizes = [1, *stack.shape[1:]]
            sizes[axis + 1] = SUB
            starts = [layer, 0, 0]
            starts[axis + 1] = sent_piece
            return lax.ppermute(lax.dynamic_slice(stack, starts, sizes)[0], 'model', MODEL_SWAP)

        def whole_weight(own, direct, axis):
            relayed = lax.ppermute(direct, 'data', CORE_SWAP)
            low = jnp.where(core == 0, direct, relayed)
            high = jnp.where(core == 0, relayed, direct)
            return jnp.concatenate([low, own, high], axis)

        order = [lax.bitwise_xor(quarter, flip) for flip in (0, 2, 1, 3)]
        mine_at, theirs_at = core * (2 * SUB), (1 - core) * (2 * SUB)
        full_cols, block_cols = 5 * SUB, 3 * SUB

        def wide_product(grad_sum, wide_inv):
            done = exact_dot(grad_sum * inv_rows, wide_inv)
            return done, lax.ppermute(done, 'data', CHIP_SWAP)

        def block_product(pieces, block_inv, is_col, earlier):
            leaving = jnp.concatenate([lax.dynamic_slice_in_dim(mat, theirs_at, 2 * SUB, 1) for mat in pieces], 0)
            staying = [lax.dynamic_slice_in_dim(mat, mine_at, 2 * SUB, 1) for mat in pieces]
            joined = jnp.concatenate(staying + [lax.ppermute(leaving, 'data', CORE_SWAP)], 0)
            rows = block_inv.shape[0] // data_ways
            block_inv = jnp.concatenate([lax.dynamic_slice_in_dim(block_inv, spot * rows, rows, 0) for spot in order], 0)
            joined = after(joined, earlier)
            share = exact_tn(joined, block_inv) if is_col else exact_tn(block_inv, joined)
            return share, lax.ppermute(share, 'data', CORE_SWAP)

        piece_one = weight_piece(w_col, 0, 1)
        piece_two = weight_piece(w_row, 0, 0)
        piece_three = weight_piece(w_col, 1, 1)
        piece_four = weight_piece(w_row, 1, 0)
        weight_one = whole_weight(w_col[0], piece_one, 1)

        edge_part = jnp.concatenate(full_gram_part(reorder(x_tokens, half)) + full_gram_part(reorder(dy_tokens, half)), 1)
        edge_sum = sum_scatter(edge_part)
        edge_all = spread(edge_sum, True)

        z_one = matmul(after(x_tokens, edge_part), weight_one).astype(jnp.bfloat16)
        h_one = activate(z_one)
        h_one_own = h_one[:, OWN]
        weight_two = whole_weight(w_row[0], after(piece_two, h_one), 0)
        early_part = jnp.concatenate(block_gram_part(h_one_own), 1)
        z_two = matmul(after(h_one, early_part, edge_sum), weight_two).astype(jnp.bfloat16)
        h_two = activate(z_two)
        weight_three = whole_weight(w_col[1], after(piece_three, h_two), 1)
        early_part = jnp.concatenate([early_part] + full_gram_part(reorder(h_two, half)), 1)
        early_sum = sum_scatter(early_part)
        z_three = matmul(after(h_two, early_part), weight_three).astype(jnp.bfloat16)
        weight_four = whole_weight(w_row[1], after(piece_four, z_three), 0)
        h_three_own = activate(z_three[:, OWN])
        dw_four_part = matmul_tn(h_three_own, dy_tokens)
        dw_four = sum_scatter(dw_four_part)
        g_three = back_gate(matmul_nt(after(dy_tokens, dw_four_part, edge_all[2]), weight_four).astype(jnp.bfloat16), z_three)
        g_three = after(g_three, early_sum, edge_all[4], edge_all[6])
        h_two_all = spread(early_sum[:, block_cols:], True)
        g_three_own = g_three[:, OWN]
        dw_three_part = matmul_tn(g_three_own, h_two)
        dw_three = sum_scatter(dw_three_part)
        middle_part = jnp.concatenate(block_gram_part(h_three_own) + block_gram_part(g_three_own), 1)
        middle_sum = sum_scatter(middle_part)
        done_four = wide_product(after(dw_four, middle_part), s_inv_row[1])
        g_two = back_gate(matmul_nt(after(g_three, dw_three_part, done_four[0]), weight_three).astype(jnp.bfloat16), z_two)
        dw_two_part = matmul_tn(h_one_own, g_two)
        dw_two = sum_scatter(dw_two_part)
        done_three = wide_product(after(dw_three, dw_two_part), a_inv_col[1])
        g_one_own = back_gate(matmul_nt(after(g_two, done_three[0], h_two_all[2]), w_row[0]).astype(jnp.bfloat16), z_one[:, OWN])
        dw_one_part = matmul_tn(g_one_own, x_tokens)
        dw_one = sum_scatter(dw_one_part)
        g_two_late = after(g_two, dw_one_part, middle_sum, done_four[1])
        mid_all = spread(middle_sum, False)
        late_part = jnp.concatenate(full_gram_part(reorder(g_two_late, half)) + block_gram_part(g_one_own), 1)
        late_sum = sum_scatter(late_part)

        new_scale = (1.0 - FACTOR_DECAY) * inv_rows

        done_two = wide_product(after(dw_two, late_part), s_inv_row[0])
        row_four = block_product(done_four, a_inv_row[1], False, done_two[0])
        spot = after(place, row_four[0])
        a_new_col = blend_layer(a_old_col, edge_all, 0, 0, new_scale, spot, None)
        s_new_row = blend_layer(s_old_row, edge_all, 5, 1, new_scale, spot, None)
        col_three = block_product(done_three, s_inv_col[1], True, after(place, a_new_col, s_new_row))
        done_one = wide_product(after(dw_one, col_three[0], a_new_col, s_new_row), a_inv_col[0])
        spot = after(place, done_one[0])
        a_new_col = blend_layer(a_old_col, h_two_all, 0, 1, new_scale, spot, a_new_col)
        a_new_row = blend_layer(a_old_row, mid_all, 0, 1, new_scale, spot, None)
        s_new_col = blend_layer(s_old_col, mid_all, 3, 1, new_scale, spot, None)
        u_row = join_layer(*row_four, 1, False, spot, None)
        u_col = join_layer(*col_three, 1, True, spot, None)
        outer_all = spread(jnp.concatenate([early_sum[:, :block_cols], late_sum[:, full_cols:]], 1), False)
        g_two_all = spread(late_sum[:, :full_cols], True)
        row_two = block_product(done_two, a_inv_row[0], False, after(place, a_new_col, u_row, u_col, late_sum))
        col_one = block_product(done_one, s_inv_col[0], True, row_two[0])
        spot = after(place, col_one[0])
        u_row = join_layer(*row_two, 0, False, spot, u_row)
        a_new_row = blend_layer(a_old_row, outer_all, 0, 0, new_scale, spot, a_new_row)
        s_new_col = blend_layer(s_old_col, outer_all, 3, 0, new_scale, spot, s_new_col)
        u_col = join_layer(*col_one, 0, True, after(spot, u_row), u_col)
        s_new_row = blend_layer(s_old_row, g_two_all, 0, 0, new_scale, after(spot, u_col), s_new_row)
        return (u_col, u_row, a_new_col, s_new_col, a_new_row, s_new_row)

    batch_split = P('data', None)
    col_split = P(None, None, 'model')
    row_split = P(None, 'model', None)
    replicated = P()
    return jax.shard_map(
        shard_body,
        mesh=mesh,
        in_specs=(batch_split, batch_split, col_split, row_split, replicated, row_split, row_split, replicated, replicated, row_split, row_split, replicated),
        out_specs=(col_split, row_split, replicated, row_split, row_split, replicated),
        check_vma=False,
    )
```

```python
import functools
import math
import jax
import jax.numpy as jnp
from jax import lax
from jax.experimental import pallas as pl
from jax.experimental.pallas import tpu as pltpu
from jax.sharding import PartitionSpec as P

FACTOR_DECAY = 0.8
GELU_SCALE = math.sqrt(2.0 / math.pi)
GELU_CUBIC = 0.044715
EXACT = lax.Precision.HIGHEST
TN_DIMS = (((0,), (0,)), ((), ()))
NT_DIMS = (((1,), (1,)), ((), ()))
SUB = 512
OWN = slice(SUB, 3 * SUB)
LOCAL_ORDER = ((2, 0, 1, 3), (1, 2, 3, 0))
MODEL_SWAP = ((0, 1), (1, 0))
CHIP_SWAP = ((0, 2), (2, 0), (1, 3), (3, 1))
CORE_SWAP = ((0, 1), (1, 0), (2, 3), (3, 2))
FULL_TABLE = ((0, 1, 0), (0, 2, 0), (0, 0, 0), (1, 4, 1),
              (0, 2, 1), (0, 3, 0), (1, 0, 1), (0, 4, 0),
              (0, 0, 1), (1, 0, 0), (1, 1, 0), (1, 2, 0),
              (1, 4, 0), (0, 4, 1), (1, 2, 1), (1, 3, 0))
BLOCK_TABLE = ((0, 0, 0), (0, 1, 0), (0, 1, 1), (0, 2, 0))


def gelu_value(pre_act):
    tanh_val = jnp.tanh(pre_act * (GELU_SCALE + (GELU_SCALE * GELU_CUBIC * pre_act) * pre_act))
    return 0.5 * pre_act * (1.0 + tanh_val)


def gelu_slope(pre_act):
    square = (3.0 * GELU_CUBIC * pre_act) * pre_act
    tanh_val = jnp.tanh(pre_act * (GELU_SCALE + (GELU_SCALE / 3.0) * square))
    upper = 0.5 + 0.5 * tanh_val
    return upper + ((upper * (1.0 - upper)) * (2.0 * GELU_SCALE * pre_act)) * (1.0 + square)


def activate(pre_act):
    return gelu_value(pre_act.astype(jnp.float32)).astype(jnp.bfloat16)


def back_gate(grad_act, pre_act):
    return (grad_act.astype(jnp.float32) * gelu_slope(pre_act.astype(jnp.float32))).astype(jnp.bfloat16)


def matmul(left_mat, right_mat):
    return jnp.dot(left_mat, right_mat, preferred_element_type=jnp.float32)


def matmul_tn(left_mat, right_mat):
    return lax.dot_general(left_mat, right_mat, TN_DIMS, preferred_element_type=jnp.float32)


def matmul_nt(left_mat, right_mat):
    return lax.dot_general(left_mat, right_mat, NT_DIMS, preferred_element_type=jnp.float32)


def exact_dot(left_mat, right_mat):
    return jnp.dot(left_mat, right_mat, precision=EXACT, preferred_element_type=jnp.float32)


def exact_tn(left_mat, right_mat):
    return lax.dot_general(left_mat, right_mat, TN_DIMS, precision=EXACT, preferred_element_type=jnp.float32)


def reorder(mat, half):
    picks = [jnp.where(half == 0, zero, one) * SUB for zero, one in zip(*LOCAL_ORDER)]
    return jnp.concatenate([lax.dynamic_slice_in_dim(mat, pick, SUB, 1) for pick in picks], 1)


def after(value, *earlier):
    return lax.optimization_barrier((value, *earlier))[0]


def full_gram_part(local_mat):
    own_a = local_mat[:, SUB:2 * SUB]
    own_b = local_mat[:, 2 * SUB:3 * SUB]
    return [matmul_tn(own_a, local_mat[:, :3 * SUB]), matmul_tn(own_b, local_mat[:, 2 * SUB:])]


def block_gram_part(own_mat):
    return [matmul_tn(own_mat[:, :SUB], own_mat), matmul_tn(own_mat[:, SUB:], own_mat[:, SUB:])]


def sum_scatter(part):
    return lax.psum_scatter(part, 'data', scatter_dimension=0, tiled=True)


def spread(piece, over_model):
    found = [piece, lax.ppermute(piece, 'data', CHIP_SWAP)]
    if over_model:
        found += [lax.ppermute(mat, 'model', MODEL_SWAP) for mat in found]
    relayed = [lax.ppermute(mat, 'data', CORE_SWAP) for mat in found]
    return [mat for pair in zip(found, relayed) for mat in pair]


def blend_body(new_scale, blocks, groups, half_tab, piece_tab, flip_tab, place, old_ref, *rest):
    piece_refs, out_ref = rest[:4 * groups], rest[-1]
    entry = pl.program_id(0) * blocks + pl.program_id(1)
    flip = flip_tab[entry]
    distance = lax.bitwise_xor(half_tab[entry], place[0]) if groups == 2 else 0
    part = SUB // 4

    def write(refs, flipped):
        for index, ref in enumerate(refs):
            spot = pl.ds(pl.multiple_of(lax.bitwise_xor(place[1], index) * part, part), part)
            if flipped:
                out_ref[0, :, spot] = FACTOR_DECAY * old_ref[0, :, spot] + new_scale * ref[...].T
            else:
                out_ref[0, spot, :] = FACTOR_DECAY * old_ref[0, spot, :] + new_scale * ref[...]

    for group in range(groups):
        for flipped in (0, 1):
            @pl.when(jnp.logical_and(flip == flipped, distance == group))
            def _():
                write(piece_refs[4 * group:4 * group + 4], flipped)


def blend_layer(old_mats, pieces, first_piece, layer, new_scale, place, partial_out):
    size = old_mats.shape[1]
    blocks = size // SUB
    groups = len(pieces) // 4
    table = FULL_TABLE if blocks == 4 else BLOCK_TABLE
    tables = [jnp.array(column, jnp.int32) for column in zip(*table)] + [place]
    spot = pl.BlockSpec((1, SUB, SUB), lambda row, col, *tabs: (layer, row, col))

    def picked(group):
        def index_map(row, col, halves, names, flips, where):
            entry = row * blocks + col
            needed = lax.bitwise_xor(halves[entry], where[0]) == group if groups == 2 else True
            return 0, first_piece + jnp.where(needed, names[entry], 0)

        return pl.BlockSpec((SUB // 4, SUB), index_map)

    in_specs = [spot] + [picked(index // 4) for index in range(len(pieces))]
    args = [old_mats, *pieces]
    aliases = {}
    if partial_out is not None:
        in_specs.append(pl.BlockSpec(memory_space=pl.ANY))
        args.append(partial_out)
        aliases = {len(tables) + len(args) - 1: 0}
    return pl.pallas_call(
        functools.partial(blend_body, new_scale, blocks, groups),
        grid_spec=pltpu.PrefetchScalarGridSpec(num_scalar_prefetch=len(tables), grid=(blocks, blocks), in_specs=in_specs, out_specs=spot),
        out_shape=jax.ShapeDtypeStruct(old_mats.shape, jnp.float32),
        input_output_aliases=aliases,
        cost_estimate=pl.CostEstimate(flops=3 * size * size, bytes_accessed=12 * size * size, transcendentals=0),
        name='blend_layer',
    )(*tables, *args)


def join_body(place, share_ref, other_ref, *rest):
    out_ref = rest[-1]
    from_share = lax.rem(place[1], 2) == pl.program_id(1)

    @pl.when(from_share)
    def _():
        out_ref[0] = share_ref[...]

    @pl.when(jnp.logical_not(from_share))
    def _():
        out_ref[0] = other_ref[...]


def join_layer(share, other, layer, is_col, place, partial_out):
    rows, cols = share.shape
    step = rows // 4
    shape = (2, 2 * rows, cols) if is_col else (2, rows, 2 * cols)
    taken = pl.BlockSpec((step, cols), lambda row, side, place: (row, 0))
    put = pl.BlockSpec((1, step, cols), lambda row, side, place: (layer, row + 4 * side, 0) if is_col else (layer, row, side))
    in_specs = [taken, taken]
    args = [share, other]
    aliases = {}
    if partial_out is not None:
        in_specs.append(pl.BlockSpec(memory_space=pl.ANY))
        args.append(partial_out)
        aliases = {3: 0}
    return pl.pallas_call(
        join_body,
        grid_spec=pltpu.PrefetchScalarGridSpec(num_scalar_prefetch=1, grid=(4, 2), in_specs=in_specs, out_specs=put),
        out_shape=jax.ShapeDtypeStruct(shape, jnp.float32),
        input_output_aliases=aliases,
        cost_estimate=pl.CostEstimate(flops=2 * rows * cols, bytes_accessed=16 * rows * cols, transcendentals=0),
        name='join_layer',
    )(place, *args)


def solution(mesh):
    data_ways = mesh.shape['data']

    def shard_body(x_tokens, dy_tokens, w_col, w_row, a_old_col, s_old_col, a_old_row, s_old_row, a_inv_col, s_inv_col, a_inv_row, s_inv_row):
        half = lax.axis_index('model')
        quarter = lax.axis_index('data')
        core = lax.rem(quarter, 2)
        inv_rows = 1.0 / (x_tokens.shape[0] * data_ways)
        sent_piece = jnp.where(core == 0, 1 - half, half) * SUB

        place = jnp.stack([half, quarter]).astype(jnp.int32)

        def weight_piece(stack, layer, axis):
            sizes = [1, *stack.shape[1:]]
            sizes[axis + 1] = SUB
            starts = [layer, 0, 0]
            starts[axis + 1] = sent_piece
            return lax.ppermute(lax.dynamic_slice(stack, starts, sizes)[0], 'model', MODEL_SWAP)

        def whole_weight(own, direct, axis):
            relayed = lax.ppermute(direct, 'data', CORE_SWAP)
            low = jnp.where(core == 0, direct, relayed)
            high = jnp.where(core == 0, relayed, direct)
            return jnp.concatenate([low, own, high], axis)

        order = [lax.bitwise_xor(quarter, flip) for flip in (0, 2, 1, 3)]
        mine_at, theirs_at = core * (2 * SUB), (1 - core) * (2 * SUB)
        full_cols, block_cols = 5 * SUB, 3 * SUB

        def wide_product(grad_sum, wide_inv):
            done = exact_dot(grad_sum * inv_rows, wide_inv)
            return done, lax.ppermute(done, 'data', CHIP_SWAP)

        def block_product(pieces, block_inv, is_col, earlier):
            leaving = jnp.concatenate([lax.dynamic_slice_in_dim(mat, theirs_at, 2 * SUB, 1) for mat in pieces], 0)
            staying = [lax.dynamic_slice_in_dim(mat, mine_at, 2 * SUB, 1) for mat in pieces]
            joined = jnp.concatenate(staying + [lax.ppermute(leaving, 'data', CORE_SWAP)], 0)
            rows = block_inv.shape[0] // data_ways
            block_inv = jnp.concatenate([lax.dynamic_slice_in_dim(block_inv, spot * rows, rows, 0) for spot in order], 0)
            joined = after(joined, earlier)
            share = exact_tn(joined, block_inv) if is_col else exact_tn(block_inv, joined)
            return share, lax.ppermute(share, 'data', CORE_SWAP)

        piece_one = weight_piece(w_col, 0, 1)
        piece_two = weight_piece(w_row, 0, 0)
        piece_three = weight_piece(w_col, 1, 1)
        piece_four = weight_piece(w_row, 1, 0)
        weight_one = whole_weight(w_col[0], piece_one, 1)

        edge_part = jnp.concatenate(full_gram_part(reorder(x_tokens, half)) + full_gram_part(reorder(dy_tokens, half)), 1)
        edge_sum = sum_scatter(edge_part)
        edge_all = spread(edge_sum, True)

        z_one = matmul(after(x_tokens, edge_part), weight_one).astype(jnp.bfloat16)
        h_one = activate(z_one)
        h_one_own = h_one[:, OWN]
        weight_two = whole_weight(w_row[0], after(piece_two, h_one), 0)
        early_part = jnp.concatenate(block_gram_part(h_one_own), 1)
        z_two = matmul(after(h_one, early_part, edge_sum), weight_two).astype(jnp.bfloat16)
        h_two = activate(z_two)
        weight_three = whole_weight(w_col[1], after(piece_three, h_two), 1)
        early_part = jnp.concatenate([early_part] + full_gram_part(reorder(h_two, half)), 1)
        early_sum = sum_scatter(early_part)
        z_three = matmul(after(h_two, early_part), weight_three).astype(jnp.bfloat16)
        weight_four = whole_weight(w_row[1], after(piece_four, z_three), 0)
        h_three_own = activate(z_three[:, OWN])
        dw_four_part = matmul_tn(h_three_own, dy_tokens)
        dw_four = sum_scatter(dw_four_part)
        g_three = back_gate(matmul_nt(after(dy_tokens, dw_four_part), weight_four).astype(jnp.bfloat16), z_three)
        g_three = after(g_three, early_sum, edge_all[2], edge_all[4])
        h_two_all = spread(early_sum[:, block_cols:], True)
        g_three_own = g_three[:, OWN]
        dw_three_part = matmul_tn(g_three_own, h_two)
        dw_three = sum_scatter(dw_three_part)
        middle_part = jnp.concatenate(block_gram_part(h_three_own) + block_gram_part(g_three_own), 1)
        middle_sum = sum_scatter(middle_part)
        done_four = wide_product(after(dw_four, middle_part), s_inv_row[1])
        g_two = back_gate(matmul_nt(after(g_three, dw_three_part, done_four[0]), weight_three).astype(jnp.bfloat16), z_two)
        dw_two_part = matmul_tn(h_one_own, g_two)
        dw_two = sum_scatter(dw_two_part)
        done_three = wide_product(after(dw_three, dw_two_part), a_inv_col[1])
        g_one_own = back_gate(matmul_nt(after(g_two, done_three[0], h_two_all[2], edge_all[6]), w_row[0]).astype(jnp.bfloat16), z_one[:, OWN])
        dw_one_part = matmul_tn(g_one_own, x_tokens)
        dw_one = sum_scatter(dw_one_part)
        g_two_late = after(g_two, dw_one_part, middle_sum, done_four[1])
        mid_all = spread(middle_sum, False)
        late_part = jnp.concatenate(full_gram_part(reorder(g_two_late, half)) + block_gram_part(g_one_own), 1)
        late_sum = sum_scatter(late_part)

        new_scale = (1.0 - FACTOR_DECAY) * inv_rows

        done_two = wide_product(after(dw_two, late_part), s_inv_row[0])
        row_four = block_product(done_four, a_inv_row[1], False, done_two[0])
        spot = after(place, row_four[0])
        a_new_col = blend_layer(a_old_col, edge_all, 0, 0, new_scale, spot, None)
        s_new_row = blend_layer(s_old_row, edge_all, 5, 1, new_scale, spot, None)
        col_three = block_product(done_three, s_inv_col[1], True, after(place, a_new_col, s_new_row))
        spot = after(place, col_three[0])
        u_row = join_layer(*row_four, 1, False, spot, None)
        u_col = join_layer(*col_three, 1, True, spot, None)
        a_new_col = blend_layer(a_old_col, h_two_all, 0, 1, new_scale, spot, a_new_col)
        a_new_row = blend_layer(a_old_row, mid_all, 0, 1, new_scale, spot, None)
        s_new_col = blend_layer(s_old_col, mid_all, 3, 1, new_scale, spot, None)
        outer_all = spread(jnp.concatenate([early_sum[:, :block_cols], late_sum[:, full_cols:]], 1), False)
        g_two_all = spread(late_sum[:, :full_cols], True)
        done_one = wide_product(after(dw_one, a_new_col, a_new_row, s_new_col, u_row, u_col), a_inv_col[0])
        row_two = block_product(done_two, a_inv_row[0], False, done_one[0])
        spot = after(place, row_two[0])
        a_new_row = blend_layer(a_old_row, outer_all, 0, 0, new_scale, spot, a_new_row)
        s_new_col = blend_layer(s_old_col, outer_all, 3, 0, new_scale, spot, s_new_col)
        u_row = join_layer(*row_two, 0, False, after(spot, a_new_row, s_new_col), u_row)
        s_new_row = blend_layer(s_old_row, g_two_all, 0, 0, new_scale, after(spot, u_row), s_new_row)
        col_one = block_product(done_one, s_inv_col[0], True, s_new_row)
        u_col = join_layer(*col_one, 0, True, place, u_col)
        return (u_col, u_row, a_new_col, s_new_col, a_new_row, s_new_row)

    batch_split = P('data', None)
    col_split = P(None, None, 'model')
    row_split = P(None, 'model', None)
    replicated = P()
    return jax.shard_map(
        shard_body,
        mesh=mesh,
        in_specs=(batch_split, batch_split, col_split, row_split, replicated, row_split, row_split, replicated, replicated, row_split, row_split, replicated),
        out_specs=(col_split, row_split, replicated, row_split, row_split, replicated),
        check_vma=False,
    )
```
